32 devices in a mesh: frames: 8 (over z, x), rows: 4 (over y, core).
Axes of the slice: x: 2, y: 2, z: 4, core: 2. Of those that a mesh axis runs over, the one named last changes fastest.
Arguments:
- fmap: bfloat16 [16, 12, 64, 128], P('frames', 'rows'), may hold values from -6 to 6
- context: bfloat16 [16, 12, 64, 128], P('frames', 'rows'), may hold values from -6 to 6
- pairs: int32 [32, 3], replicated, may hold values from 0 to 15, as said below
- w_corr: bfloat16 [49, 128], replicated, may hold values from -0.875 to 0.875
- w_zr: bfloat16 [256, 256], replicated, may hold values from -0.375 to 0.375
- w_q: bfloat16 [9, 256, 128], replicated, may hold values from -0.125 to 0.125
- w_msg: bfloat16 [128, 256], replicated, may hold values from -0.5 to 0.5
- w_res: bfloat16 [9, 128, 128], replicated, may hold values from -0.1875 to 0.1875
Outputs:
- state: bfloat16 [16, 12, 64, 128], P('frames', 'rows')
The draws below stay inside these ranges and needn't reach their ends.
Inputs may be any that keep to these rules, and one draw needn't show every extreme that they name: Source and target differ. With dev(f) = f // 2, the source's dev, the target's dev and the owner differ pairwise by at most one. No owner holds more than 8 pairs, and some owner holds exactly 8.
All inputs are finite; a program needn't handle non-finite values.
Results may differ from the reference program's by a relative error of at most 0.01.
Values may be sent and summed in bfloat16 or wider, within the bound.
A program may use at most 64 MiB of HBM per device.

```python
import jax
import jax.numpy as jnp

CHANNELS = 128
IMG_WIDTH = 64
FRAME_DEV = 2
PAIR_DEV = 4
RADIUS = 3
ROUNDS = 2
FRAMES = 16
IMG_HEIGHT = 12
PAIR_TOTAL = 32
N_FRAMES = 8


def draw_pairs(key, part):
    keys = jax.random.split(jax.random.fold_in(key, 71), 9)
    halves = N_FRAMES // 2
    capacity = 2 * PAIR_DEV
    loads = jax.random.randint(keys[0], (halves,), 0, capacity + 1).astype(jnp.int32)
    forced = jax.random.randint(keys[1], (), 1, halves - 1).astype(jnp.int32)
    half_ids = jnp.arange(halves, dtype=jnp.int32)
    loads = jnp.where(half_ids == forced, capacity, loads).astype(jnp.int32)
    flips = jax.random.randint(keys[2], (halves,), 0, 2).astype(jnp.int32)
    evens = jnp.where(flips == 1, loads, capacity - loads).astype(jnp.int32)
    evens = jnp.where(half_ids == halves - 1, jnp.maximum(evens, 1), evens).astype(jnp.int32)
    evens = jnp.where(half_ids == 0, jnp.minimum(evens, capacity - 1), evens).astype(jnp.int32)
    counts = jnp.stack([evens, capacity - evens], axis=1).reshape(N_FRAMES).astype(jnp.int32)
    ends = jnp.cumsum(counts).astype(jnp.int32)
    positions = jnp.arange(PAIR_TOTAL, dtype=jnp.int32)
    owners = jnp.sum((positions[:, None] >= ends[None, :]).astype(jnp.int32), axis=1).astype(jnp.int32)
    src_step = jax.random.randint(keys[3], (PAIR_TOTAL,), -1, 2).astype(jnp.int32)
    src_dev = jnp.clip(owners + src_step, 0, N_FRAMES - 1).astype(jnp.int32)
    tgt_step = jax.random.randint(keys[4], (PAIR_TOTAL,), -1, 2).astype(jnp.int32)
    picker = jax.random.randint(keys[5], (PAIR_TOTAL,), 0, 2).astype(jnp.int32)
    tgt_dev = jnp.where(src_dev == owners, jnp.clip(owners + tgt_step, 0, N_FRAMES - 1), jnp.where(picker == 0, owners, src_dev)).astype(jnp.int32)
    high_first = ends[N_FRAMES - 3]
    low_first = ends[0]
    src_dev = jnp.where(positions == high_first, N_FRAMES - 2, src_dev).astype(jnp.int32)
    tgt_dev = jnp.where(positions == high_first, N_FRAMES - 1, tgt_dev).astype(jnp.int32)
    src_dev = jnp.where(positions == low_first, 0, src_dev).astype(jnp.int32)
    tgt_dev = jnp.where(positions == low_first, 1, tgt_dev).astype(jnp.int32)
    sources = (src_dev * FRAME_DEV + jax.random.randint(keys[6], (PAIR_TOTAL,), 0, FRAME_DEV)).astype(jnp.int32)
    targets = (tgt_dev * FRAME_DEV + jax.random.randint(keys[7], (PAIR_TOTAL,), 0, FRAME_DEV)).astype(jnp.int32)
    other = (src_dev * FRAME_DEV + (sources % FRAME_DEV + 1) % FRAME_DEV).astype(jnp.int32)
    targets = jnp.where(targets == sources, other, targets).astype(jnp.int32)
    table = jnp.stack([sources, targets, owners], axis=1).astype(jnp.int32)
    order = jax.random.permutation(keys[8], PAIR_TOTAL)
    return jnp.take(table, order, axis=0).astype(jnp.int32)


def shard_levels(rng, dims, shards, least, top_value):
    loudness = 1.0
    for dim, parts in shards:
        steps = jax.random.uniform(jax.random.fold_in(jax.random.fold_in(rng, 6), dim), (parts,), jnp.float32, least / len(shards), top_value / len(shards))
        loudness = loudness * jnp.repeat(jnp.exp(steps), dims[dim] // parts).reshape((-1,) + (1,) * (len(dims) - 1 - dim))
    return loudness


def bell_draw(key, extent, deviation, reach, shards=(), kind=jnp.bfloat16):
    array = jax.random.normal(key, extent, jnp.float32) * deviation
    if len(shards) > 0:
        array = shard_levels(key, extent, shards, -0.22, 0.18) * array
    return jnp.clip(array, min=-reach, max=reach).astype(kind)


def setup_inputs(seed: int = 0) -> dict:
    arg_keys = jax.random.split(jax.random.key(seed), 9)
    return {
        "fmap": bell_draw(arg_keys[0], (FRAMES, IMG_HEIGHT, IMG_WIDTH, CHANNELS), 1.0, 6.0, ((0, 8), (1, 4))),
        "context": bell_draw(arg_keys[1], (FRAMES, IMG_HEIGHT, IMG_WIDTH, CHANNELS), 1.0, 6.0, ((0, 8), (1, 4))),
        "pairs": draw_pairs(jax.random.fold_in(arg_keys[8], 71), 0),
        "w_corr": bell_draw(arg_keys[3], ((2 * RADIUS + 1) ** 2, CHANNELS), ((2 * RADIUS + 1) ** 2) ** -0.5, 0.875),
        "w_zr": bell_draw(arg_keys[4], (2 * CHANNELS, 2 * CHANNELS), (2 * CHANNELS) ** -0.5, 0.375),
        "w_q": bell_draw(arg_keys[5], (9, 2 * CHANNELS, CHANNELS), (18 * CHANNELS) ** -0.5, 0.125),
        "w_msg": bell_draw(arg_keys[6], (CHANNELS, 2 * CHANNELS), CHANNELS ** -0.5, 0.5),
        "w_res": bell_draw(arg_keys[7], (9, CHANNELS, CHANNELS), (9 * CHANNELS) ** -0.5, 0.1875),
    }


def conv_three(padded, kernel, height, width):
    count = padded.shape[0]
    cin = padded.shape[-1]
    total = None
    for row_off in range(3):
        for col_off in range(3):
            window = padded[:, row_off:row_off + height, col_off:col_off + width, :].reshape(-1, cin)
            term = jnp.dot(window, kernel[3 * row_off + col_off], preferred_element_type=jnp.float32)
            total = term if total is None else total + term
    return total.reshape(count, height, width, -1)


def pad_both(field, amount):
    return jnp.pad(field, ((0, 0), (amount, amount), (amount, amount), (0, 0)))


def reference(fmap, context, pairs, w_corr, w_zr, w_q, w_msg, w_res):
    sources = pairs[:, 0].astype(jnp.int32)
    targets = pairs[:, 1].astype(jnp.int32)
    height = fmap.shape[1]
    width = fmap.shape[2]
    chans = fmap.shape[3]
    span = 2 * RADIUS + 1
    src_feat = jnp.take(fmap, sources, axis=0).astype(jnp.float32)
    tgt_pad = pad_both(jnp.take(fmap, targets, axis=0), RADIUS)
    columns = []
    for row_off in range(span):
        for col_off in range(span):
            moved = tgt_pad[:, row_off:row_off + height, col_off:col_off + width, :].astype(jnp.float32)
            columns.append(jnp.einsum('pyxc,pyxc->pyx', src_feat, moved))
    scale = 1.0 / (chans ** 0.5)
    corr = (jnp.stack(columns, axis=-1) * scale).astype(jnp.bfloat16)
    motion = jax.nn.relu(jnp.dot(corr.reshape(-1, span * span), w_corr, preferred_element_type=jnp.float32))
    motion = motion.astype(jnp.bfloat16).reshape(-1, height, width, chans)
    state = context
    hidden = None
    for sweep in range(ROUNDS):
        ctx_src = jnp.take(state, sources, axis=0).astype(jnp.float32)
        if sweep == 0:
            hidden = jnp.tanh(ctx_src)
        xin = (motion.astype(jnp.float32) + ctx_src).astype(jnp.bfloat16)
        joined = jnp.concatenate([hidden.astype(jnp.bfloat16), xin], axis=-1)
        gates = jax.nn.sigmoid(jnp.dot(joined.reshape(-1, 2 * chans), w_zr, preferred_element_type=jnp.float32))
        gates = gates.reshape(-1, height, width, 2 * chans)
        update_gate = gates[..., :chans]
        reset_gate = gates[..., chans:]
        qin = jnp.concatenate([(reset_gate * hidden).astype(jnp.bfloat16), xin], axis=-1)
        candidate = jnp.tanh(conv_three(pad_both(qin, 1), w_q, height, width))
        hidden = (1.0 - update_gate) * hidden + update_gate * candidate
        messages = jnp.dot(hidden.astype(jnp.bfloat16).reshape(-1, chans), w_msg, preferred_element_type=jnp.float32)
        messages = messages.astype(jnp.bfloat16).reshape(-1, height, width, 2 * chans)
        incoming = jax.ops.segment_sum(messages[..., :chans].astype(jnp.float32), sources, num_segments=FRAMES)
        incoming = incoming + jax.ops.segment_sum(messages[..., chans:].astype(jnp.float32), targets, num_segments=FRAMES)
        update = jax.nn.relu(incoming).astype(jnp.bfloat16)
        state = (state.astype(jnp.float32) + conv_three(pad_both(update, 1), w_res, height, width)).astype(jnp.bfloat16)
    return state
```

```python
import functools

import jax
import jax.numpy as jnp
from jax import lax
from jax.experimental import pallas as pl
from jax.experimental.pallas import tpu as pltpu
from jax.sharding import PartitionSpec as P

RADIUS = 3
ROUNDS = 2
CAPACITY = 8
LANES = 128
MESH = pl.DeviceIdType.MESH
F32 = jnp.float32
BF16 = jnp.bfloat16
LEFT, RIGHT, UP, DOWN = range(4)


def dot(a, b):
    return jnp.dot(a, b, preferred_element_type=F32)


def dot_nt(a, b):
    return lax.dot_general(a, b, (((1,), (1,)), ((), ())), preferred_element_type=F32)


def kernel(
    nf, nr,
    pairs_ref, fmap_ref, ctx_ref, wcorr_ref, wzr_ref, wq_ref, wmsg_ref, wres_ref,
    out_ref,
    fwin, cwin, motion, hid, zbuf, qr, qx, msend, mrecv, mown, ubuf, sbuf,
    wsel, wq_s, wres_s, wmsg_s, tbl,
    ssem, rsem, lsem,
):
    f = lax.axis_index("frames")
    r = lax.axis_index("rows")
    fd, height, width, chans = fmap_ref.shape
    npair = pairs_ref.shape[0]
    rows = height * width
    has = {LEFT: f > 0, RIGHT: f < nf - 1, UP: r > 0, DOWN: r < nr - 1}
    dev = {LEFT: (f - 1, r), RIGHT: (f + 1, r), UP: (f, r - 1), DOWN: (f, r + 1)}
    back = {LEFT: RIGHT, RIGHT: LEFT, UP: DOWN, DOWN: UP}
    sent = []

    def rcopy(i, way, src, dst):
        return pltpu.make_async_remote_copy(
            src_ref=src, dst_ref=dst, send_sem=ssem.at[i], recv_sem=rsem.at[i],
            device_id=dev[way], device_id_type=MESH,
        )

    def push(i, way, src, dst, cond=None):
        cond = has[way] if cond is None else jnp.logical_and(cond, has[way])
        sent.append((i, way, src, dst, cond))

        @pl.when(cond)
        def _():
            rcopy(i, way, src, dst).start()

    def arrive(i, way, src, dst, cond=None):
        cond = has[back[way]] if cond is None else jnp.logical_and(cond, has[back[way]])

        @pl.when(cond)
        def _():
            rcopy(i, way, src, dst).wait_recv()

    own_rows = pl.ds(RADIUS, height)
    place = {RIGHT: pl.ds(0, fd), LEFT: pl.ds(2 * fd, fd)}
    middle = pl.ds(fd, fd)

    own_f = pltpu.make_async_copy(fmap_ref, fwin.at[middle, own_rows], lsem.at[0])
    own_c = pltpu.make_async_copy(ctx_ref, cwin.at[0, middle], lsem.at[1])
    own_f.start()
    own_c.start()

    barrier = pltpu.get_barrier_semaphore()
    count = 0
    for way in (LEFT, RIGHT, UP, DOWN):
        count = count + has[way].astype(jnp.int32)

        @pl.when(has[way])
        def _(way=way):
            pl.semaphore_signal(barrier, inc=1, device_id=dev[way], device_id_type=MESH)

    pl.semaphore_wait(barrier, count)

    for way in (RIGHT, LEFT):
        push(way, way, fmap_ref, fwin.at[place[way], own_rows])
    edge_src = {UP: pl.ds(RADIUS, RADIUS), DOWN: pl.ds(height, RADIUS)}
    edge_dst = {UP: pl.ds(RADIUS + height, RADIUS), DOWN: pl.ds(0, RADIUS)}
    feat_edge = {UP: pl.ds(0, RADIUS), DOWN: pl.ds(height - RADIUS, RADIUS)}
    for way in (UP, DOWN):
        push(way, way, fmap_ref.at[:, feat_edge[way]], fwin.at[middle, edge_dst[way]])
    for way in (RIGHT, LEFT):
        push(4 + way, way, ctx_ref, cwin.at[0, place[way]])

    fwin[:, 2 * RADIUS + height] = jnp.zeros(
        (fwin.shape[0],) + fwin.shape[2:], BF16
    )

    @pl.when(r == 0)
    def _():
        fwin[:, 0:RADIUS] = jnp.zeros((fwin.shape[0], RADIUS, width, chans), BF16)
        for k in range(ROUNDS):
            qr[k, :, 0] = jnp.zeros((CAPACITY, width, chans), BF16)
            qx[k, :, 0] = jnp.zeros((CAPACITY, width, chans), BF16)
            ubuf[k, :, 0] = jnp.zeros((fd, width, chans), BF16)

    @pl.when(r == nr - 1)
    def _():
        fwin[:, RADIUS + height : 2 * RADIUS + height] = jnp.zeros(
            (fwin.shape[0], RADIUS, width, chans), BF16
        )
        for k in range(ROUNDS):
            qr[k, :, height + 1] = jnp.zeros((CAPACITY, width, chans), BF16)
            qx[k, :, height + 1] = jnp.zeros((CAPACITY, width, chans), BF16)
            ubuf[k, :, height + 1] = jnp.zeros((fd, width, chans), BF16)

    for way, edge in ((RIGHT, f == 0), (LEFT, f == nf - 1)):
        @pl.when(edge)
        def _(way=way):
            fwin[place[way]] = jnp.zeros((fd,) + fwin.shape[1:], BF16)
            for k in range(ROUNDS):
                cwin[k, place[way]] = jnp.zeros((fd, height, width, chans), BF16)
                mrecv[k, way] = jnp.zeros((fd, rows, chans), BF16)

    zero = jnp.int32(0)

    def pick(p, carry):
        seen, srcs, tgts, ok = carry
        mine = (pairs_ref[p, 2] == f).astype(jnp.int32)
        s, t = pairs_ref[p, 0], pairs_ref[p, 1]
        hits = [mine * (seen == k).astype(jnp.int32) for k in range(CAPACITY)]
        srcs = tuple(v + h * s for v, h in zip(srcs, hits))
        tgts = tuple(v + h * t for v, h in zip(tgts, hits))
        ok = tuple(v + h for v, h in zip(ok, hits))
        return seen + mine, srcs, tgts, ok

    zeros = (zero,) * CAPACITY
    _, srcs, tgts, oks = lax.fori_loop(0, npair, pick, (zero, zeros, zeros, zeros))
    first = (f - 1) * fd
    last = 3 * fd - 1
    for k in range(CAPACITY):
        s_idx = jnp.clip(srcs[k] - first, 0, last)
        t_idx = jnp.clip(tgts[k] - first, 0, last)
        tbl[0, k] = s_idx
        tbl[1, k] = t_idx
        tbl[2, k] = jnp.where(oks[k] == 1, s_idx, -1)
        tbl[3, k] = jnp.where(oks[k] == 1, t_idx, -1)

    span = 2 * RADIUS + 1
    per = LANES // width
    groups = (span + per - 1) // per
    depth = groups * LANES
    line = lax.broadcasted_iota(jnp.int32, (depth, wcorr_ref.shape[0]), 0)
    col = lax.broadcasted_iota(jnp.int32, (depth, wcorr_ref.shape[0]), 1)
    lane = lax.rem(line, LANES) + RADIUS + 1
    b_off = lax.rem(lane, width)
    a_off = lax.div(line, LANES) * per + lax.rem(lax.div(lane, width) + per - 1, per)
    take = jnp.logical_and(b_off < span, a_off < span)
    index = jnp.where(take, a_off * span + b_off, -1)
    wsel[...] = dot(
        jnp.where(index == col, 1.0, 0.0).astype(BF16), wcorr_ref[...]
    ).astype(BF16)
    for k in range(3):
        for j in range(3):
            wq_s[k, :, j * chans : (j + 1) * chans] = wq_ref[3 * k + j]
            wres_s[k, :, j * chans : (j + 1) * chans] = wres_ref[3 * k + j]
    wmsg_s[0:chans] = wmsg_ref[:, 0:chans]
    wmsg_s[chans : 2 * chans] = wmsg_ref[:, chans : 2 * chans]

    own_f.wait()
    for way in (RIGHT, LEFT):
        arrive(way, way, fmap_ref, fwin.at[place[way], own_rows])
        for n, side in enumerate((UP, DOWN)):
            push(
                8 + 2 * way + n, side, fwin.at[place[way], edge_src[side]],
                fwin.at[place[way], edge_dst[side]], cond=has[back[way]],
            )
    for side in (UP, DOWN):
        arrive(side, side, fmap_ref.at[:, feat_edge[side]], fwin.at[middle, edge_dst[side]])
    for way in (RIGHT, LEFT):
        for n, side in enumerate((UP, DOWN)):
            arrive(
                8 + 2 * way + n, side, fwin.at[place[way], edge_src[side]],
                fwin.at[place[way], edge_dst[side]], cond=has[back[way]],
            )

    xs = width - 1 - lax.broadcasted_iota(jnp.int32, (width, LANES), 0)
    ls = lax.broadcasted_iota(jnp.int32, (width, LANES), 1) + RADIUS + 1
    bs = lax.rem(ls, width)
    flip = jnp.where(
        lax.broadcasted_iota(jnp.int32, (width, width), 0)
        + lax.broadcasted_iota(jnp.int32, (width, width), 1)
        == width - 1,
        1.0,
        0.0,
    ).astype(BF16)
    inside = jnp.logical_and(xs + bs >= RADIUS, xs + bs < width + RADIUS)
    inside = jnp.logical_and(inside, bs < span)
    scale = 1.0 / chans**0.5

    @pl.loop(0, CAPACITY)
    def _(s):
        src_i, tgt_i = tbl[0, s], tbl[1, s]
        lines = []
        for y in range(height):
            a = dot(flip, fwin[src_i, RADIUS + y]).astype(BF16)
            b = fwin[tgt_i, pl.ds(y, groups * per)].reshape(groups * per * width, chans)
            g = dot_nt(a, b) * scale
            tiles = []
            for j in range(groups):
                tile = pltpu.roll(
                    g[:, j * LANES : (j + 1) * LANES], 0, 1, stride=1, stride_axis=0
                )
                tiles.append(jnp.where(inside, tile, 0.0).astype(BF16))
            lines.append(jnp.concatenate(tiles, axis=1))
        corr = jnp.concatenate(lines, axis=0)
        moved = jnp.maximum(dot(corr, wsel[...]), 0.0).astype(BF16)
        for y in range(height):
            motion[s, y * width : (y + 1) * width] = dot(
                flip, moved[y * width : (y + 1) * width]
            ).astype(BF16)

    own_c.wait()
    for way in (RIGHT, LEFT):
        arrive(4 + way, way, ctx_ref, cwin.at[0, place[way]])

    line_no = lax.rem(lax.broadcasted_iota(jnp.int32, (rows, chans), 0), width)
    not_first = line_no > 0
    not_last = line_no < width - 1

    def shifted_sum(acc):
        before = pltpu.roll(acc[:, 0:chans], 1, 0)
        after = pltpu.roll(acc[:, 2 * chans : 3 * chans], rows - 1, 0)
        return (
            jnp.where(not_first, before, 0.0)
            + acc[:, chans : 2 * chans]
            + jnp.where(not_last, after, 0.0)
        )

    halo_src = {UP: 1, DOWN: height}
    halo_dst = {UP: height + 1, DOWN: 0}

    for k in range(ROUNDS):
        base = 16 + 16 * k

        @pl.loop(0, CAPACITY)
        def _(s):
            state = cwin[k, tbl[0, s]].reshape(rows, chans).astype(F32)
            if k == 0:
                hid[s] = jnp.tanh(state)
            xin = (motion[s].astype(F32) + state).astype(BF16)
            qx[k, s, pl.ds(1, height)] = xin.reshape(height, width, chans)

        for n, side in enumerate((UP, DOWN)):
            push(base + n, side, qx.at[k, :, halo_src[side]], qx.at[k, :, halo_dst[side]])

        @pl.loop(0, CAPACITY)
        def _(s):
            h = hid[s]
            xin = qx[k, s, pl.ds(1, height)].reshape(rows, chans)
            gates = jax.nn.sigmoid(dot(jnp.concatenate([h.astype(BF16), xin], axis=1), wzr_ref[...]))
            zbuf[s] = gates[:, 0:chans]
            qr[k, s, pl.ds(1, height)] = (
                (gates[:, chans : 2 * chans] * h).astype(BF16).reshape(height, width, chans)
            )

        for n, side in enumerate((UP, DOWN)):
            push(base + 2 + n, side, qr.at[k, :, halo_src[side]], qr.at[k, :, halo_dst[side]])
        for n, side in enumerate((UP, DOWN)):
            arrive(base + n, side, qx.at[k, :, halo_src[side]], qx.at[k, :, halo_dst[side]])
            arrive(base + 2 + n, side, qr.at[k, :, halo_src[side]], qr.at[k, :, halo_dst[side]])

        @pl.loop(0, CAPACITY)
        def _(s):
            acc = None
            for dy in range(3):
                part = jnp.concatenate(
                    [
                        qr[k, s, pl.ds(dy, height)].reshape(rows, chans),
                        qx[k, s, pl.ds(dy, height)].reshape(rows, chans),
                    ],
                    axis=1,
                )
                term = dot(part, wq_s[dy])
                acc = term if acc is None else acc + term
            cand = jnp.tanh(shifted_sum(acc))
            z = zbuf[s]
            hid[s] = (1.0 - z) * hid[s] + z * cand

        def message(j):
            first_sum = jnp.zeros((rows, chans), F32)
            second_sum = jnp.zeros((rows, chans), F32)
            for s in range(CAPACITY):
                h = hid[s]
                first_sum = first_sum + jnp.where(tbl[2, s] == j, 1.0, 0.0) * h
                second_sum = second_sum + jnp.where(tbl[3, s] == j, 1.0, 0.0) * h
            both = jnp.concatenate([first_sum.astype(BF16), second_sum.astype(BF16)], axis=1)
            return dot(both, wmsg_s[...])

        for way, start in ((LEFT, 0), (RIGHT, 2 * fd)):
            @pl.loop(0, fd)
            def _(j, way=way, start=start):
                msend[k, way, j] = message(start + j).astype(BF16)

            push(base + 4 + way, way, msend.at[k, way], mrecv.at[k, way])

        @pl.loop(0, fd)
        def _(j):
            mown[j] = message(fd + j)

        for way in (LEFT, RIGHT):
            arrive(base + 4 + way, way, msend.at[k, way], mrecv.at[k, way])

        @pl.loop(0, fd)
        def _(j):
            total = mown[j] + mrecv[k, LEFT, j].astype(F32) + mrecv[k, RIGHT, j].astype(F32)
            ubuf[k, j, pl.ds(1, height)] = (
                jnp.maximum(total, 0.0).astype(BF16).reshape(height, width, chans)
            )

        for n, side in enumerate((UP, DOWN)):
            push(base + 8 + n, side, ubuf.at[k, :, halo_src[side]], ubuf.at[k, :, halo_dst[side]])
        for n, side in enumerate((UP, DOWN)):
            arrive(base + 8 + n, side, ubuf.at[k, :, halo_src[side]], ubuf.at[k, :, halo_dst[side]])

        @pl.loop(0, fd)
        def _(j):
            acc = None
            for dy in range(3):
                term = dot(ubuf[k, j, pl.ds(dy, height)].reshape(rows, chans), wres_s[dy])
                acc = term if acc is None else acc + term
            old = cwin[k, fd + j].reshape(rows, chans).astype(F32)
            new = (old + shifted_sum(acc)).astype(BF16).reshape(height, width, chans)
            if k == ROUNDS - 1:
                out_ref[j] = new
            else:
                sbuf[k, j] = new
                cwin[k + 1, fd + j] = new

        if k < ROUNDS - 1:
            for way in (RIGHT, LEFT):
                push(base + 12 + way, way, sbuf.at[k], cwin.at[k + 1, place[way]])
            for way in (RIGHT, LEFT):
                arrive(base + 12 + way, way, sbuf.at[k], cwin.at[k + 1, place[way]])

    for i, way, src, dst, cond in sent:
        @pl.when(cond)
        def _(i=i, way=way, src=src, dst=dst):
            rcopy(i, way, src, dst).wait_send()


def local(nf, nr, fmap, context, pairs, w_corr, w_zr, w_q, w_msg, w_res):
    fd, height, width, chans = fmap.shape
    rows = height * width
    win = 3 * fd
    groups = -(-(2 * RADIUS + 1) // (LANES // width))
    vmem = pl.BlockSpec(memory_space=pltpu.VMEM)
    return pl.pallas_call(
        functools.partial(kernel, nf, nr),
        out_shape=jax.ShapeDtypeStruct(fmap.shape, BF16),
        in_specs=[pl.BlockSpec(memory_space=pltpu.SMEM)] + [vmem] * 7,
        out_specs=vmem,
        scratch_shapes=[
            pltpu.VMEM((win, 2 * RADIUS + height + 1, width, chans), BF16),
            pltpu.VMEM((ROUNDS, win, height, width, chans), BF16),
            pltpu.VMEM((CAPACITY, rows, chans), BF16),
            pltpu.VMEM((CAPACITY, rows, chans), F32),
            pltpu.VMEM((CAPACITY, rows, chans), F32),
            pltpu.VMEM((ROUNDS, CAPACITY, height + 2, width, chans), BF16),
            pltpu.VMEM((ROUNDS, CAPACITY, height + 2, width, chans), BF16),
            pltpu.VMEM((ROUNDS, 2, fd, rows, chans), BF16),
            pltpu.VMEM((ROUNDS, 2, fd, rows, chans), BF16),
            pltpu.VMEM((fd, rows, chans), F32),
            pltpu.VMEM((ROUNDS, fd, height + 2, width, chans), BF16),
            pltpu.VMEM((ROUNDS, fd, height, width, chans), BF16),
            pltpu.VMEM((groups * LANES, chans), BF16),
            pltpu.VMEM((3, 2 * chans, 3 * chans), BF16),
            pltpu.VMEM((3, chans, 3 * chans), BF16),
            pltpu.VMEM((2 * chans, chans), BF16),
            pltpu.SMEM((4, CAPACITY), jnp.int32),
            pltpu.SemaphoreType.DMA((16 + 16 * ROUNDS,)),
            pltpu.SemaphoreType.DMA((16 + 16 * ROUNDS,)),
            pltpu.SemaphoreType.DMA((2,)),
        ],
        compiler_params=pltpu.CompilerParams(collective_id=0, has_side_effects=True),
    )(pairs, fmap, context, w_corr, w_zr, w_q, w_msg, w_res)


def solution(mesh):
    placed = (P("frames", "rows", None, None), P("frames", "rows", None, None)) + (P(),) * 6
    return jax.shard_map(
        functools.partial(local, mesh.shape["frames"], mesh.shape["rows"]),
        mesh=mesh,
        in_specs=placed,
        out_specs=P("frames", "rows", None, None),
        check_vma=False,
    )
```

```python
import functools

import jax
import jax.numpy as jnp
from jax import lax
from jax.experimental import pallas as pl
from jax.experimental.pallas import tpu as pltpu
from jax.sharding import PartitionSpec as P

RADIUS = 3
ROUNDS = 2
CAPACITY = 8
LANES = 128
MESH = pl.DeviceIdType.MESH
F32 = jnp.float32
BF16 = jnp.bfloat16
LEFT, RIGHT, UP, DOWN = range(4)


def dot(a, b):
    return jnp.dot(a, b, preferred_element_type=F32)


def dot_nt(a, b):
    return lax.dot_general(a, b, (((1,), (1,)), ((), ())), preferred_element_type=F32)


def kernel(
    nf, nr,
    pairs_ref, fmap_ref, ctx_ref, wcorr_ref, wzr_ref, wq_ref, wmsg_ref, wres_ref,
    out_ref,
    fwin, cwin, motion, hid, zbuf, qr, qx, msend, mrecv, mown, ubuf, sbuf,
    wsel, wq_s, wres_s, wmsg_s, pre, rim, tbl,
    ssem, rsem, lsem,
):
    f = lax.axis_index("frames")
    r = lax.axis_index("rows")
    fd, height, width, chans = fmap_ref.shape
    npair = pairs_ref.shape[0]
    rows = height * width
    has = {LEFT: f > 0, RIGHT: f < nf - 1, UP: r > 0, DOWN: r < nr - 1}
    dev = {LEFT: (f - 1, r), RIGHT: (f + 1, r), UP: (f, r - 1), DOWN: (f, r + 1)}
    back = {LEFT: RIGHT, RIGHT: LEFT, UP: DOWN, DOWN: UP}
    sent = []

    def both(cond, gate):
        return cond if gate is None else jnp.logical_and(cond, gate)

    def rcopy(handle):
        i, way, src, dst, _ = handle
        return pltpu.make_async_remote_copy(
            src_ref=src, dst_ref=dst, send_sem=ssem.at[i], recv_sem=rsem.at[i],
            device_id=dev[way], device_id_type=MESH,
        )

    def push(way, src, dst, gate=None):
        handle = (len(sent), way, src, dst, gate)
        sent.append(handle)

        @pl.when(both(has[way], gate))
        def _():
            rcopy(handle).start()

        return handle

    def arrive(handle):
        @pl.when(both(has[back[handle[1]]], handle[4]))
        def _():
            rcopy(handle).wait_recv()

    own_rows = pl.ds(RADIUS, height)
    place = {RIGHT: pl.ds(0, fd), LEFT: pl.ds(2 * fd, fd)}
    middle = pl.ds(fd, fd)

    own_f = pltpu.make_async_copy(fmap_ref, fwin.at[middle, own_rows], lsem.at[0])
    own_c = pltpu.make_async_copy(ctx_ref, cwin.at[0, middle], lsem.at[1])
    loads = []
    for k in range(3):
        for j in range(3):
            lanes = pl.ds(j * chans, chans)
            loads.append((wq_ref.at[3 * k + j], wq_s.at[k, :, lanes]))
            loads.append((wres_ref.at[3 * k + j], wres_s.at[k, :, lanes]))
    loads = [
        pltpu.make_async_copy(src, dst, lsem.at[2 + n]) for n, (src, dst) in enumerate(loads)
    ]

    barrier = pltpu.get_barrier_semaphore()
    count = 0
    for way in (LEFT, RIGHT, UP, DOWN):
        count = count + has[way].astype(jnp.int32)

        @pl.when(has[way])
        def _(way=way):
            pl.semaphore_signal(barrier, inc=1, device_id=dev[way], device_id_type=MESH)

    own_f.start()
    own_c.start()
    for load in loads:
        load.start()
    pl.semaphore_wait(barrier, count)

    seat = {RIGHT: 0, LEFT: 2 * fd}
    feats = {}
    for j in range(fd):
        for way in (RIGHT, LEFT):
            feats[way, j] = push(way, fmap_ref.at[j], fwin.at[seat[way] + j, own_rows])
    edge_src = {UP: pl.ds(RADIUS, RADIUS), DOWN: pl.ds(height, RADIUS)}
    edge_dst = {UP: pl.ds(RADIUS + height, RADIUS), DOWN: pl.ds(0, RADIUS)}
    feat_edge = {UP: pl.ds(0, RADIUS), DOWN: pl.ds(height - RADIUS, RADIUS)}
    edges = [
        push(way, fmap_ref.at[:, feat_edge[way]], fwin.at[middle, edge_dst[way]])
        for way in (UP, DOWN)
    ]
    states = [push(way, ctx_ref, cwin.at[0, place[way]]) for way in (RIGHT, LEFT)]

    fwin[:, 2 * RADIUS + height] = jnp.zeros(
        (fwin.shape[0],) + fwin.shape[2:], BF16
    )

    @pl.when(r == 0)
    def _():
        fwin[:, 0:RADIUS] = jnp.zeros((fwin.shape[0], RADIUS, width, chans), BF16)
        for k in range(ROUNDS):
            qr[k, :, 0] = jnp.zeros((CAPACITY, width, chans), BF16)
            qx[k, :, 0] = jnp.zeros((CAPACITY, width, chans), BF16)
            ubuf[k, :, 0] = jnp.zeros((fd, width, chans), BF16)

    @pl.when(r == nr - 1)
    def _():
        fwin[:, RADIUS + height : 2 * RADIUS + height] = jnp.zeros(
            (fwin.shape[0], RADIUS, width, chans), BF16
        )
        for k in range(ROUNDS):
            qr[k, :, height + 1] = jnp.zeros((CAPACITY, width, chans), BF16)
            qx[k, :, height + 1] = jnp.zeros((CAPACITY, width, chans), BF16)
            ubuf[k, :, height + 1] = jnp.zeros((fd, width, chans), BF16)

    for way, edge in ((RIGHT, f == 0), (LEFT, f == nf - 1)):
        @pl.when(edge)
        def _(way=way):
            fwin[place[way]] = jnp.zeros((fd,) + fwin.shape[1:], BF16)
            for k in range(ROUNDS):
                cwin[k, place[way]] = jnp.zeros((fd, height, width, chans), BF16)
                mrecv[k, way] = jnp.zeros((fd, rows, chans), BF16)

    zero = jnp.int32(0)

    def pick(p, carry):
        seen, srcs, tgts, ok = carry
        mine = (pairs_ref[p, 2] == f).astype(jnp.int32)
        s, t = pairs_ref[p, 0], pairs_ref[p, 1]
        hits = [mine * (seen == k).astype(jnp.int32) for k in range(CAPACITY)]
        srcs = tuple(v + h * s for v, h in zip(srcs, hits))
        tgts = tuple(v + h * t for v, h in zip(tgts, hits))
        ok = tuple(v + h for v, h in zip(ok, hits))
        return seen + mine, srcs, tgts, ok

    zeros = (zero,) * CAPACITY
    _, srcs, tgts, oks = lax.fori_loop(0, npair, pick, (zero, zeros, zeros, zeros))
    first = (f - 1) * fd
    last = 3 * fd - 1
    for k in range(CAPACITY):
        s_idx = jnp.clip(srcs[k] - first, 0, last)
        t_idx = jnp.clip(tgts[k] - first, 0, last)
        tbl[0, k] = s_idx
        tbl[1, k] = t_idx
        tbl[2, k] = jnp.where(oks[k] == 1, s_idx, -1)
        tbl[3, k] = jnp.where(oks[k] == 1, t_idx, -1)

    span = 2 * RADIUS + 1
    per = LANES // width
    groups = (span + per - 1) // per
    depth = groups * LANES
    line = lax.broadcasted_iota(jnp.int32, (depth, wcorr_ref.shape[0]), 0)
    col = lax.broadcasted_iota(jnp.int32, (depth, wcorr_ref.shape[0]), 1)
    lane = lax.rem(line, LANES) + RADIUS + 1
    b_off = lax.rem(lane, width)
    a_off = lax.div(line, LANES) * per + lax.rem(lax.div(lane, width) + per - 1, per)
    take = jnp.logical_and(b_off < span, a_off < span)
    index = jnp.where(take, a_off * span + b_off, -1)
    wsel[...] = dot(
        jnp.where(index == col, 1.0, 0.0).astype(BF16), wcorr_ref[...]
    ).astype(BF16)
    wmsg_s[0:chans] = wmsg_ref[:, 0:chans]
    wmsg_s[chans : 2 * chans] = wmsg_ref[:, chans : 2 * chans]

    own_f.wait()
    for j in range(fd):
        for way in (RIGHT, LEFT):
            arrive(feats[way, j])
            spot = seat[way] + j
            for side in (UP, DOWN):
                edges.append(
                    push(
                        side, fwin.at[spot, edge_src[side]], fwin.at[spot, edge_dst[side]],
                        gate=has[back[way]],
                    )
                )
    for handle in edges:
        arrive(handle)

    xs = width - 1 - lax.broadcasted_iota(jnp.int32, (width, LANES), 0)
    ls = lax.broadcasted_iota(jnp.int32, (width, LANES), 1) + RADIUS + 1
    bs = lax.rem(ls, width)
    flip = jnp.where(
        lax.broadcasted_iota(jnp.int32, (width, width), 0)
        + lax.broadcasted_iota(jnp.int32, (width, width), 1)
        == width - 1,
        1.0,
        0.0,
    ).astype(BF16)
    inside = jnp.logical_and(xs + bs >= RADIUS, xs + bs < width + RADIUS)
    inside = jnp.logical_and(inside, bs < span)
    scale = 1.0 / chans**0.5

    @pl.loop(0, CAPACITY, unroll=4)
    def _(s):
        src_i, tgt_i = tbl[0, s], tbl[1, s]
        lines = []
        for y in range(height):
            a = dot(flip, fwin[src_i, RADIUS + y]).astype(BF16)
            b = fwin[tgt_i, pl.ds(y, groups * per)].reshape(groups * per * width, chans)
            g = dot_nt(a, b) * scale
            tiles = []
            for j in range(groups):
                tile = pltpu.roll(
                    g[:, j * LANES : (j + 1) * LANES], 0, 1, stride=1, stride_axis=0
                )
                tiles.append(jnp.where(inside, tile, 0.0).astype(BF16))
            lines.append(jnp.concatenate(tiles, axis=1))
        corr = jnp.concatenate(lines, axis=0)
        moved = jnp.maximum(dot(corr, wsel[...]), 0.0).astype(BF16)
        for y in range(height):
            motion[s, y * width : (y + 1) * width] = dot(
                flip, moved[y * width : (y + 1) * width]
            ).astype(BF16)

    own_c.wait()
    for load in loads:
        load.wait()

    def shifted_sum(acc):
        rows = acc.shape[0]
        line_no = lax.rem(lax.broadcasted_iota(jnp.int32, (rows, chans), 0), width)
        not_first = line_no > 0
        not_last = line_no < width - 1
        before = pltpu.roll(acc[:, 0:chans], 1, 0)
        after = pltpu.roll(acc[:, 2 * chans : 3 * chans], rows - 1, 0)
        return (
            jnp.where(not_first, before, 0.0)
            + acc[:, chans : 2 * chans]
            + jnp.where(not_last, after, 0.0)
        )

    def conv_own(part, weight):
        blank = jnp.zeros((width, 3 * chans), F32)
        acc = dot(part, weight[1])
        if height > 1:
            acc = acc + jnp.concatenate([blank, dot(part[: rows - width], weight[0])], axis=0)
            acc = acc + jnp.concatenate([dot(part[width:], weight[2]), blank], axis=0)
        return shifted_sum(acc)

    halo_src = {UP: 1, DOWN: height}
    halo_dst = {UP: height + 1, DOWN: 0}

    for k in range(ROUNDS):
        for handle in states:
            arrive(handle)

        @pl.loop(0, CAPACITY, unroll=4)
        def _(s):
            state = cwin[k, tbl[0, s]].reshape(rows, chans).astype(F32)
            if k == 0:
                hid[s] = jnp.tanh(state)
            xin = (motion[s].astype(F32) + state).astype(BF16)
            qx[k, s, pl.ds(1, height)] = xin.reshape(height, width, chans)

        halos = [
            push(side, qx.at[k, :, halo_src[side]], qx.at[k, :, halo_dst[side]])
            for side in (UP, DOWN)
        ]

        @pl.loop(0, CAPACITY, unroll=4)
        def _(s):
            h = hid[s]
            xin = qx[k, s, pl.ds(1, height)].reshape(rows, chans)
            gates = jax.nn.sigmoid(dot(jnp.concatenate([h.astype(BF16), xin], axis=1), wzr_ref[...]))
            zbuf[s] = gates[:, 0:chans]
            qr[k, s, pl.ds(1, height)] = (
                (gates[:, chans : 2 * chans] * h).astype(BF16).reshape(height, width, chans)
            )

        halos += [
            push(side, qr.at[k, :, halo_src[side]], qr.at[k, :, halo_dst[side]])
            for side in (UP, DOWN)
        ]

        @pl.loop(0, CAPACITY, unroll=4)
        def _(s):
            part = jnp.concatenate(
                [
                    qr[k, s, pl.ds(1, height)].reshape(rows, chans),
                    qx[k, s, pl.ds(1, height)].reshape(rows, chans),
                ],
                axis=1,
            )
            pre[s] = conv_own(part, wq_s)

        for handle in halos:
            arrive(handle)
        for n, (line_at, tap) in enumerate(((0, 0), (height + 1, 2))):
            part = jnp.concatenate(
                [
                    qr[k, :, line_at].reshape(CAPACITY * width, chans),
                    qx[k, :, line_at].reshape(CAPACITY * width, chans),
                ],
                axis=1,
            )
            rim[n] = shifted_sum(dot(part, wq_s[tap])).reshape(CAPACITY, width, chans)

        @pl.loop(0, CAPACITY, unroll=4)
        def _(s):
            for y in range(height):
                piece = pl.ds(y * width, width)
                total = pre[s, piece]
                if y == 0:
                    total = total + rim[0, s]
                if y == height - 1:
                    total = total + rim[1, s]
                z = zbuf[s, piece]
                hid[s, piece] = (1.0 - z) * hid[s, piece] + z * jnp.tanh(total)

        def message(j):
            first_sum = jnp.zeros((rows, chans), F32)
            second_sum = jnp.zeros((rows, chans), F32)
            for s in range(CAPACITY):
                h = hid[s]
                first_sum = first_sum + jnp.where(tbl[2, s] == j, 1.0, 0.0) * h
                second_sum = second_sum + jnp.where(tbl[3, s] == j, 1.0, 0.0) * h
            both = jnp.concatenate([first_sum.astype(BF16), second_sum.astype(BF16)], axis=1)
            return dot(both, wmsg_s[...])

        parcels = []
        for j in range(fd):
            for way, start in ((LEFT, 0), (RIGHT, 2 * fd)):
                msend[k, way, j] = message(start + j).astype(BF16)
                parcels.append(push(way, msend.at[k, way, j], mrecv.at[k, way, j]))
        for j in range(fd):
            mown[j] = message(fd + j)
        for handle in parcels:
            arrive(handle)
        for j in range(fd):
            total = mown[j] + mrecv[k, LEFT, j].astype(F32) + mrecv[k, RIGHT, j].astype(F32)
            ubuf[k, j, pl.ds(1, height)] = (
                jnp.maximum(total, 0.0).astype(BF16).reshape(height, width, chans)
            )
        halos = [
            push(side, ubuf.at[k, :, halo_src[side]], ubuf.at[k, :, halo_dst[side]])
            for side in (UP, DOWN)
        ]
        for j in range(fd):
            part = ubuf[k, j, pl.ds(1, height)].reshape(rows, chans)
            mown[j] = cwin[k, fd + j].reshape(rows, chans).astype(F32) + conv_own(part, wres_s)
        for handle in halos:
            arrive(handle)
        states = []
        for j in range(fd):
            top = shifted_sum(dot(ubuf[k, j, 0], wres_s[0]))
            bottom = shifted_sum(dot(ubuf[k, j, height + 1], wres_s[2]))
            for y in range(height):
                total = mown[j, y * width : (y + 1) * width]
                if y == 0:
                    total = total + top
                if y == height - 1:
                    total = total + bottom
                if k == ROUNDS - 1:
                    out_ref[j, y] = total.astype(BF16)
                else:
                    sbuf[k, j, y] = total.astype(BF16)
                    cwin[k + 1, fd + j, y] = total.astype(BF16)
            if k < ROUNDS - 1:
                for way in (RIGHT, LEFT):
                    states.append(push(way, sbuf.at[k, j], cwin.at[k + 1, seat[way] + j]))

    for handle in sent:
        @pl.when(both(has[handle[1]], handle[4]))
        def _(handle=handle):
            rcopy(handle).wait_send()


def local(nf, nr, fmap, context, pairs, w_corr, w_zr, w_q, w_msg, w_res):
    fd, height, width, chans = fmap.shape
    rows = height * width
    win = 3 * fd
    groups = -(-(2 * RADIUS + 1) // (LANES // width))
    copies = 6 * fd + 4 + ROUNDS * (6 + 2 * fd) + (ROUNDS - 1) * 2 * fd
    vmem = pl.BlockSpec(memory_space=pltpu.VMEM)
    hbm = pl.BlockSpec(memory_space=pl.ANY)
    return pl.pallas_call(
        functools.partial(kernel, nf, nr),
        out_shape=jax.ShapeDtypeStruct(fmap.shape, BF16),
        in_specs=[
            pl.BlockSpec(memory_space=pltpu.SMEM), vmem, vmem, vmem, vmem, hbm, vmem, hbm,
        ],
        out_specs=vmem,
        scratch_shapes=[
            pltpu.VMEM((win, 2 * RADIUS + height + 1, width, chans), BF16),
            pltpu.VMEM((ROUNDS, win, height, width, chans), BF16),
            pltpu.VMEM((CAPACITY, rows, chans), BF16),
            pltpu.VMEM((CAPACITY, rows, chans), F32),
            pltpu.VMEM((CAPACITY, rows, chans), F32),
            pltpu.VMEM((ROUNDS, CAPACITY, height + 2, width, chans), BF16),
            pltpu.VMEM((ROUNDS, CAPACITY, height + 2, width, chans), BF16),
            pltpu.VMEM((ROUNDS, 2, fd, rows, chans), BF16),
            pltpu.VMEM((ROUNDS, 2, fd, rows, chans), BF16),
            pltpu.VMEM((fd, rows, chans), F32),
            pltpu.VMEM((ROUNDS, fd, height + 2, width, chans), BF16),
            pltpu.VMEM((ROUNDS, fd, height, width, chans), BF16),
            pltpu.VMEM((groups * LANES, chans), BF16),
            pltpu.VMEM((3, 2 * chans, 3 * chans), BF16),
            pltpu.VMEM((3, chans, 3 * chans), BF16),
            pltpu.VMEM((2 * chans, chans), BF16),
            pltpu.VMEM((CAPACITY, rows, chans), F32),
            pltpu.VMEM((2, CAPACITY, width, chans), F32),
            pltpu.SMEM((4, CAPACITY), jnp.int32),
            pltpu.SemaphoreType.DMA((copies,)),
            pltpu.SemaphoreType.DMA((copies,)),
            pltpu.SemaphoreType.DMA((20,)),
        ],
        compiler_params=pltpu.CompilerParams(collective_id=0, has_side_effects=True),
    )(pairs, fmap, context, w_corr, w_zr, w_q, w_msg, w_res)


def solution(mesh):
    placed = (P("frames", "rows", None, None), P("frames", "rows", None, None)) + (P(),) * 6
    return jax.shard_map(
        functools.partial(local, mesh.shape["frames"], mesh.shape["rows"]),
        mesh=mesh,
        in_specs=placed,
        out_specs=P("frames", "rows", None, None),
        check_vma=False,
    )
```
